32 devices in a mesh: expert: 4 (over y, core), shard: 8 (over z, x).
Axes of the slice: x: 2, y: 2, z: 4, core: 2. Of those that a mesh axis runs over, the one named last changes fastest.
Arguments:
- hidden_in: bfloat16 [12288, 1536], P(('expert', 'shard')), may hold values from -6 to 6
- cotangent: bfloat16 [12288, 1536], P(('expert', 'shard')), may hold values from -6 to 6
- routes: int32 [12288, 8], P(('expert', 'shard')), may hold values from 0 to 19, all different within a row; in each aligned block of 384 rows (0 to 383, 384 to 767, ...) at most 256 rows name the same one
- attn_gain: bfloat16 [1536], P('shard'), may hold values from 0.5 to 1.5
- q_weight: bfloat16 [1536, 1536], P('shard'), may hold values from -0.21875 to 0.21875
- k_weight: bfloat16 [1536, 512], P('shard'), may hold values from -0.21875 to 0.21875
- v_weight: bfloat16 [1536, 512], P('shard'), may hold values from -0.15625 to 0.15625
- o_weight: bfloat16 [1536, 1536], P('shard'), may hold values from -1 to 1
- ffn_gain: bfloat16 [1536], P('shard'), may hold values from 0.5 to 1.5
- router_weight: bfloat16 [1536, 20], P('shard'), may hold values from -0.078125 to 0.078125
- gate_weight: bfloat16 [20, 1536, 512], P('expert', 'shard'), may hold values from -0.15625 to 0.15625
- up_weight: bfloat16 [20, 1536, 512], P('expert', 'shard'), may hold values from -0.15625 to 0.15625
- down_weight: bfloat16 [20, 512, 1536], P('expert', 'shard'), may hold values from -1.5 to 1.5
Outputs:
- hidden_out: bfloat16 [12288, 1536], P(('expert', 'shard'))
- grad_hidden: bfloat16 [12288, 1536], P(('expert', 'shard'))
- grad_attn_gain: float32 [1536], P('shard')
- grad_q: float32 [1536, 1536], P('shard')
- grad_k: float32 [1536, 512], P('shard')
- grad_v: float32 [1536, 512], P('shard')
- grad_o: float32 [1536, 1536], P('shard')
- grad_ffn_gain: float32 [1536], P('shard')
- grad_router: float32 [1536, 20], P('shard')
- grad_gate: float32 [20, 1536, 512], P('expert', 'shard')
- grad_up: float32 [20, 1536, 512], P('expert', 'shard')
- grad_down: float32 [20, 512, 1536], P('expert', 'shard')
The draws below stay inside these ranges and needn't reach their ends.
Inputs may be any that keep to these rules, and one draw needn't show every extreme that they name: In the 384 rows of one device no expert is named by more than 256 routes, and in every draw some expert is named by exactly 256 there; the routes of a row are distinct.
All inputs are finite; a program needn't handle non-finite values.
Results may differ from the reference program's by a relative error of at most 0.025.
Values may be sent and summed in bfloat16 or wider, within the bound.
A program may use at most 320 MiB of HBM per device.

```python
import math
import jax
import jax.numpy as jnp
import numpy as np
from jax import lax

D = 1536
HQ = 24
KV = 8
HS = 64
FF = 512
TOP = 8
PR_DEV = 128
CONT = 512
HALF = 256
TOK_DEV = 384
PROMPT = 1024
TOKENS = 12288
EXPERTS = 20
CAP = 256
N_EXPERT = 4
N_SHARD = 8


def steps_of(own_key, dims, split, smallest, largest):
    def one(position, parts):
        draws = jax.random.uniform(jax.random.fold_in(jax.random.fold_in(own_key, 6), position), (parts,), jnp.float32, smallest / len(split), largest / len(split))
        return jnp.repeat(jnp.exp(draws), dims[position] // parts).reshape((-1,) + (1,) * (len(dims) - position - 1))

    gain = one(*split[0])
    for cut in split[1:]:
        gain = gain * one(*cut)
    return gain


def assign_block(rng, own, number, rows, number_of, top, limit, lean):
    sequence = jax.random.permutation(rng, number_of)
    crowded, common = load_shares(number_of, rows * top, limit, lean, True), load_shares(number_of, rows * top, limit, lean, False)
    places = jnp.arange(number_of)

    def named(lengths, offset_by):
        used = int((lengths > 0).sum())
        fixed = max(1, used // 4)
        passed = fixed + (places - fixed + offset_by * (used - fixed)) % max(1, number_of - fixed)
        return jnp.zeros((number_of,), jnp.int32).at[sequence[jnp.where(places < fixed, places, passed)]].set(jnp.asarray(lengths, jnp.int32))

    lengths = jnp.where(number % 4 == 0, named(crowded, number // 4), named(common, number - number // 4 - 1))
    mixed = jax.random.permutation(jax.random.fold_in(own, 3), number_of)
    source_of, taker = mixed[0:number_of // 2 * 2:2], mixed[1:number_of // 2 * 2:2]
    slack = jnp.minimum(lengths[source_of] - 1, limit - lengths[taker]) // 2
    slack = jnp.where((source_of == sequence[0]) | (taker == sequence[0]) | (lengths[taker] == 0), 0, jnp.maximum(slack, 0))
    passed = jax.random.randint(jax.random.fold_in(own, 4), (number_of // 2,), 0, 1 << 20) % (slack + 1)
    lengths = lengths.at[source_of].add(-passed).at[taker].add(passed)
    members = jnp.searchsorted(jnp.cumsum(lengths), jnp.arange(rows * top), side="right").astype(jnp.int32)
    grid = members.reshape(top, rows).T
    grid = grid[jax.random.permutation(jax.random.fold_in(own, 1), rows)]
    offset_by = jax.random.randint(jax.random.fold_in(own, 2), (rows, 1), 0, top)
    return jnp.take_along_axis(grid, (jnp.arange(top)[None, :] + offset_by) % top, axis=1)


def load_shares(count, total, limit, skew, full):
    portions = [(1 << 20) // math.isqrt(rank ** skew) + 1 for rank in range(1, count + 1)]
    largest = limit if full else min(limit, max(-(-total // count), total * portions[0] // sum(portions)))
    least = 1 if total - largest >= count - 1 else 0
    given, spare = [largest] + [least] * (count - 1), total - largest - least * (count - 1)
    while spare > 0:
        free = [i for i in range(1, count) if given[i] < largest] or [i for i in range(1, count) if given[i] < limit]
        whole, remaining = sum([portions[i] for i in free]), spare
        for i in free:
            addition = min(limit - given[i], max(1, remaining * portions[i] // whole), spare)
            given[i] = given[i] + addition
            spare = spare - addition
    return np.array(given)


def scatter_about(key, dims, width, bound, cuts=(), kind=jnp.bfloat16):
    values = jax.random.normal(key, dims, jnp.float32) * width
    if len(cuts) > 0:
        values = steps_of(key, dims, cuts, -0.22, 0.18) * values
    return jnp.clip(values, min=-bound, max=bound).astype(kind)


def setup_inputs(seed: int = 0) -> dict:
    splits = jax.random.split(jax.random.key(seed), 14)
    hidden_in = scatter_about(splits[0], (TOKENS, D), 1.0, 6.0, ((0, 32),))
    cotangent = scatter_about(splits[1], (TOKENS, D), 1.0, 6.0, ((0, 32),))
    routes_keys = jax.random.split(jax.random.fold_in(splits[2], 1), TOKENS // TOK_DEV)
    routes_turns = jax.random.permutation(jax.random.fold_in(splits[2], 3), TOKENS // TOK_DEV)
    routes = jax.vmap(lambda own, number: assign_block(jax.random.fold_in(splits[2], 2), own, number, TOK_DEV, EXPERTS, TOP, CAP, 1))(routes_keys, routes_turns).reshape((TOKENS, TOP))
    attn_gain = jnp.clip(1.0 + 0.1 * jax.random.normal(splits[3], (D,), jnp.float32), 0.5, 1.5).astype(jnp.bfloat16)
    q_weight = scatter_about(splits[4], (D, HQ * HS), (D // 2) ** -0.5, 0.21875, ((0, 8),))
    k_weight = scatter_about(splits[5], (D, KV * HS), (D // 2) ** -0.5, 0.21875, ((0, 8),))
    v_weight = scatter_about(splits[6], (D, KV * HS), D ** -0.5, 0.15625, ((0, 8),))
    o_weight = scatter_about(splits[7], (HQ * HS, D), (HQ * HS // 48) ** -0.5, 1.0, ((0, 8),))
    ffn_gain = jnp.clip(1.0 + 0.1 * jax.random.normal(splits[8], (D,), jnp.float32), 0.5, 1.5).astype(jnp.bfloat16)
    router_weight = scatter_about(splits[9], (D, EXPERTS), (4 * D) ** -0.5, 0.078125, ((0, 8),))
    gate_weight = scatter_about(splits[10], (EXPERTS, D, FF), D ** -0.5, 0.15625, ((0, 4), (1, 8)))
    up_weight = scatter_about(splits[11], (EXPERTS, D, FF), D ** -0.5, 0.15625, ((0, 4), (1, 8)))
    down_weight = scatter_about(splits[12], (EXPERTS, FF, D), (FF // 32) ** -0.5, 1.5, ((0, 4), (1, 8)))
    return dict(hidden_in=hidden_in, cotangent=cotangent, routes=routes, attn_gain=attn_gain, q_weight=q_weight, k_weight=k_weight, v_weight=v_weight, o_weight=o_weight, ffn_gain=ffn_gain, router_weight=router_weight, gate_weight=gate_weight, up_weight=up_weight, down_weight=down_weight)


epsilon = 1e-05
negative = -1e+30
highest = lax.Precision.HIGHEST

@jax.custom_vjp
def low(v):
    return lax.optimization_barrier(v.astype(jnp.bfloat16)).astype(jnp.float32)

@jax.custom_vjp
def low_back(v):
    return v

def low_keep(v):
    return (low(v), None)

def low_pass(kept, grad):
    return (grad,)

def back_keep(v):
    return (v, None)

def back_low(kept, grad):
    return (low(grad),)
low.defvjp(low_keep, low_pass)
low_back.defvjp(back_keep, back_low)

def matmul(left, right):
    return jnp.dot(left, right, precision=highest, preferred_element_type=jnp.float32)

def rms_norm(values, gain_row):
    return values * lax.rsqrt(lax.optimization_barrier(jnp.mean(values * values, -1, keepdims=True)) + epsilon) * gain_row

def rotate_half(values):
    middle = values.shape[-1] // 2
    return jnp.concatenate([-values[..., middle:], values[..., :middle]], -1)

def rope_tables(positions, head_size):
    inv_freq = 10000.0 ** (-jnp.arange(head_size // 2, dtype=jnp.float32) * 2.0 / head_size)
    angles = positions.astype(jnp.float32)[:, None] * inv_freq[None, :]
    angles = jnp.concatenate([angles, angles], -1)
    return (jnp.cos(angles), jnp.sin(angles))

def rope_apply(values, cosine_table, sine_table):
    return values * cosine_table[:, None, :] + rotate_half(values) * sine_table[:, None, :]

def positions_all():
    block_rows = jnp.arange(TOK_DEV, dtype=jnp.int32)
    shard_pos = jnp.arange(N_EXPERT * N_SHARD, dtype=jnp.int32) % N_SHARD
    prompt_pos = shard_pos[:, None] * PR_DEV + block_rows[None, :]
    cont_pos = PROMPT + 2 * (block_rows[None, :] - PR_DEV) + shard_pos[:, None] % 2
    return jnp.where(block_rows[None, :] < PR_DEV, prompt_pos, cont_pos).reshape(-1)

def split_group(array):
    tail_shape = array.shape[1:]
    blocks = array.reshape((N_SHARD, TOK_DEV) + tail_shape)
    prompt_part = blocks[:, :PR_DEV].reshape((PROMPT,) + tail_shape)
    cont_part = blocks[:, PR_DEV:].reshape((N_SHARD // 2, 2, HALF) + tail_shape)
    cont_part = jnp.swapaxes(cont_part, 1, 2).reshape((N_SHARD // 2, CONT) + tail_shape)
    return (prompt_part, cont_part)

def join_group(prompt_part, cont_part):
    tail_shape = prompt_part.shape[1:]
    prompt_blocks = prompt_part.reshape((N_SHARD, PR_DEV) + tail_shape)
    cont_blocks = jnp.swapaxes(cont_part.reshape((N_SHARD // 2, HALF, 2) + tail_shape), 1, 2)
    cont_blocks = cont_blocks.reshape((N_SHARD, HALF) + tail_shape)
    return jnp.concatenate([prompt_blocks, cont_blocks], 1).reshape((N_SHARD * TOK_DEV,) + tail_shape)

def head_attention(operands):
    query_prompt, query_cont, key_prompt, key_cont, value_prompt, value_cont = operands
    score_scale = HS ** (-0.5)
    prompt_index = jnp.arange(PROMPT)
    cont_index = jnp.arange(CONT)
    scores_pp = low_back(jnp.einsum('pgs,ks->gpk', query_prompt, key_prompt, precision=highest) * score_scale)
    scores_pp = jnp.where((prompt_index[:, None] >= prompt_index[None, :])[None], scores_pp, negative)
    probs_pp = low(jax.nn.softmax(scores_pp, -1))
    out_prompt = jnp.einsum('gpk,ks->pgs', probs_pp, value_prompt, precision=highest)
    scores_cp = low_back(jnp.einsum('clgs,ks->cglk', query_cont, key_prompt, precision=highest) * score_scale)
    scores_cc = low_back(jnp.einsum('clgs,cjs->cglj', query_cont, key_cont, precision=highest) * score_scale)
    scores_cc = jnp.where((cont_index[:, None] >= cont_index[None, :])[None, None], scores_cc, negative)
    probs_cont = low(jax.nn.softmax(jnp.concatenate([scores_cp, scores_cc], -1), -1))
    out_cont = jnp.einsum('cglk,ks->clgs', probs_cont[..., :PROMPT], value_prompt, precision=highest)
    out_cont = out_cont + jnp.einsum('cglj,cjs->clgs', probs_cont[..., PROMPT:], value_cont, precision=highest)
    return (out_prompt, out_cont)

def group_attention(operands):
    queries, key_rows, value_rows = operands
    group_size = HQ // KV
    query_prompt, query_cont = split_group(queries.reshape(-1, KV, group_size, HS))
    key_prompt, key_cont = split_group(key_rows)
    value_prompt, value_cont = split_group(value_rows)
    per_head = (jnp.moveaxis(query_prompt, 1, 0), jnp.moveaxis(query_cont, 2, 0), jnp.moveaxis(key_prompt, 1, 0), jnp.moveaxis(key_cont, 2, 0), jnp.moveaxis(value_prompt, 1, 0), jnp.moveaxis(value_cont, 2, 0))
    out_prompt, out_cont = lax.map(jax.checkpoint(head_attention), per_head)
    out_prompt = jnp.moveaxis(out_prompt, 0, 1).reshape(PROMPT, HQ * HS)
    out_cont = jnp.moveaxis(out_cont, 0, 2).reshape(N_SHARD // 2, CONT, HQ * HS)
    return join_group(out_prompt, out_cont)

def block_experts(operands, gate_weight, up_weight, down_weight):
    rows_in, block_routes, block_gates = operands
    flat_routes = block_routes.reshape(-1).astype(jnp.int32)
    route_hits = (flat_routes[:, None] == jnp.arange(EXPERTS, dtype=jnp.int32)[None, :]).astype(jnp.int32)
    slot_index = lax.optimization_barrier(jnp.sum((jnp.cumsum(route_hits, 0) - 1) * route_hits, 1)).astype(jnp.int32)
    destination = (flat_routes * CAP + slot_index).astype(jnp.int32)
    route_token = (jnp.arange(TOK_DEV * TOP, dtype=jnp.int32) // TOP).astype(jnp.int32)
    slot_token = jnp.zeros(EXPERTS * CAP, jnp.int32).at[destination].set(route_token)
    slot_used = jnp.zeros(EXPERTS * CAP, jnp.float32).at[destination].set(1.0)
    buffer = low_back(rows_in[slot_token] * slot_used[:, None]).reshape(EXPERTS, CAP, D)
    gate_proj = low_back(jnp.einsum('ecd,edf->ecf', buffer, gate_weight, precision=highest))
    up_proj = low_back(jnp.einsum('ecd,edf->ecf', buffer, up_weight, precision=highest))
    inner_act = low(jax.nn.silu(gate_proj) * up_proj)
    expert_out = low(low_back(jnp.einsum('ecf,efd->ecd', inner_act, down_weight, precision=highest)))
    picked = expert_out.reshape(EXPERTS * CAP, D)[destination].reshape(TOK_DEV, TOP, D)
    return lax.optimization_barrier(jnp.sum(picked * block_gates[:, :, None], 1))

def forward(hidden, attn_gain, q_weight, k_weight, v_weight, o_weight, ffn_gain, router_weight, gate_weight, up_weight, down_weight, routes, cosine_table, sine_table):
    row_count = hidden.shape[0]
    attn_input = low(rms_norm(hidden, attn_gain))
    queries = low(rope_apply(low_back(matmul(attn_input, q_weight)).reshape(row_count, HQ, HS), cosine_table, sine_table))
    key_rows = low(rope_apply(low_back(matmul(attn_input, k_weight)).reshape(row_count, KV, HS), cosine_table, sine_table))
    value_rows = low(low_back(matmul(attn_input, v_weight))).reshape(row_count, KV, HS)
    attn_mix = lax.map(group_attention, (queries.reshape(N_EXPERT, -1, HQ, HS), key_rows.reshape(N_EXPERT, -1, KV, HS), value_rows.reshape(N_EXPERT, -1, KV, HS)))
    attn_mix = low(low_back(attn_mix.reshape(row_count, HQ * HS)))
    residual = hidden + low_back(matmul(attn_mix, o_weight))
    ffn_input = low(rms_norm(residual, ffn_gain))
    logits = low_back(matmul(ffn_input, router_weight))
    route_gates = jax.nn.softmax(jnp.take_along_axis(logits, routes, 1), -1)

    def expert_block(operands):
        return block_experts(operands, gate_weight, up_weight, down_weight)
    moe_out = lax.map(jax.checkpoint(expert_block), (ffn_input.reshape(N_EXPERT * N_SHARD, TOK_DEV, D), routes.reshape(N_EXPERT * N_SHARD, TOK_DEV, TOP), route_gates.reshape(N_EXPERT * N_SHARD, TOK_DEV, TOP)))
    return residual + moe_out.reshape(row_count, D)

def reference(hidden_in, cotangent, routes, attn_gain, q_weight, k_weight, v_weight, o_weight, ffn_gain, router_weight, gate_weight, up_weight, down_weight):
    cosine_table, sine_table = rope_tables(positions_all(), HS)

    def run_layer(*weights):
        return forward(*weights, routes, cosine_table, sine_table)
    floats = tuple((item.astype(jnp.float32) for item in (hidden_in, attn_gain, q_weight, k_weight, v_weight, o_weight, ffn_gain, router_weight, gate_weight, up_weight, down_weight)))
    output, pullback = jax.vjp(run_layer, *floats)
    gradients = pullback(cotangent.astype(jnp.float32))
    return (output.astype(jnp.bfloat16), gradients[0].astype(jnp.bfloat16), gradients[1], gradients[2], gradients[3], gradients[4], gradients[5], gradients[6], gradients[7], gradients[8], gradients[9], gradients[10])
```

```python
import functools

import jax
import jax.numpy as jnp
from jax import lax
from jax.experimental import pallas as pl
from jax.experimental.pallas import tpu as pltpu
from jax.sharding import Mesh
from jax.sharding import PartitionSpec as P

HS = 64
PR_DEV = 128

epsilon = 1e-05
negative = -1e30
bf16 = jnp.bfloat16
f32 = jnp.float32
EXPERT = ("y", "c")
SHARD = ("z", "x")


def other(block, axis):
    return lax.ppermute(block, axis, [(0, 1), (1, 0)])


def pick(flag, when_one, when_zero):
    return jnp.where(flag == 1, when_one, when_zero)


def all_pairs():
    return all(lax.axis_size(axis) == 2 for axis in ("y", "c", "x"))


def gather_experts(block):
    if not all_pairs():
        return lax.all_gather(block, EXPERT, axis=0)
    pair = jnp.stack([block, other(block, "y")])
    return jnp.concatenate([pair, other(pair, "c")], 0)


def spread_experts(blocks):
    if not all_pairs():
        return lax.all_to_all(blocks, EXPERT, split_axis=0, concat_axis=0, tiled=True)
    here = lax.axis_index(EXPERT)

    def at(apart):
        return lax.dynamic_index_in_dim(blocks, here ^ apart, 0, keepdims=False)

    across = other(jnp.stack([at(2), at(3)]), "y")
    far = other(jnp.stack([at(1), across[1]]), "c")
    return jnp.stack([at(0), across[0], far[0], far[1]])


def absolute_order(stacked):
    count = stacked.shape[0]
    if not all_pairs():
        return [stacked[place] for place in range(count)]
    here = lax.axis_index(EXPERT)
    slot_of = [0, 2, 1, 3]
    table = jnp.array(slot_of, jnp.int32)
    return [
        lax.dynamic_index_in_dim(stacked, table[here ^ place], 0, keepdims=False)
        for place in range(count)
    ]


def gather_tokens(block):
    if not all_pairs():
        return lax.all_gather(block, EXPERT + ("x",), axis=0, tiled=True)
    half = block.shape[0] // 2
    from_x, from_y = other(block, "x"), other(block, "y")
    near = [block, from_x, from_y, other(from_x[:half], "y"), other(from_y[half:], "x")]
    return jnp.concatenate(near + [other(piece, "c") for piece in near], 0)


def reduce_tokens(partial, count):
    if not all_pairs():
        return lax.psum_scatter(
            partial(0, count), EXPERT + ("x",), scatter_dimension=0, tiled=True
        ).astype(f32)
    rows = count // 8
    far = other(partial(4 * rows, count), "c")
    near = partial(0, 4 * rows)
    half = rows // 2

    def piece(place, start):
        part = slice(place * rows + start, place * rows + start + half)
        return near[part].astype(f32) + far[part].astype(f32)

    def sent(value, axis):
        return other(value.astype(bf16), axis).astype(f32)

    across_x, across_y = sent(piece(3, 0), "x"), sent(piece(3, half), "y")
    own_x, own_y = sent(piece(1, 0), "x"), sent(piece(2, half), "y")
    first = piece(0, 0) + own_x + sent(piece(2, 0) + across_x, "y")
    second = piece(0, half) + own_y + sent(piece(1, half) + across_y, "x")
    return jnp.concatenate([first, second], 0)


def rotated(values):
    width = values.shape[-1]
    lane = lax.broadcasted_iota(jnp.int32, values.shape, values.ndim - 1)
    low = lane % HS < HS // 2
    return jnp.where(
        low, -jnp.roll(values, -(HS // 2), -1), jnp.roll(values, HS // 2, -1)
    )


def rope_tables(positions, width):
    inv_freq = 10000.0 ** (-jnp.arange(HS // 2, dtype=f32) * 2.0 / HS)
    inv_freq = jnp.tile(inv_freq, width // (HS // 2))
    angles = positions.astype(f32)[:, None] * inv_freq[None, :]
    return jnp.cos(angles), jnp.sin(angles)


def norm_rows(values, gain_row):
    inverse = lax.rsqrt(jnp.mean(values * values, -1, keepdims=True) + epsilon)
    normed = values * inverse
    return normed, inverse, normed * gain_row


def norm_back(grad_out, normed, inverse, gain_row):
    scaled = grad_out * gain_row
    grad_in = inverse * (scaled - normed * jnp.mean(scaled * normed, -1, keepdims=True))
    return grad_in, jnp.sum(grad_out * normed, 0)


def nt(left, right):
    return lax.dot_general(left, right, (((1,), (1,)), ((), ())), preferred_element_type=f32)


def nn(left, right):
    return jnp.dot(left, right, preferred_element_type=f32)


def tn(left, right):
    return lax.dot_general(left, right, (((0,), (0,)), ((), ())), preferred_element_type=f32)


def masked_scores(place, keys, query, rows, first_row, prompt_len, half_len):
    if first_row == 0:
        scores = nt(keys[:prompt_len], query)
        key = lax.broadcasted_iota(jnp.int32, scores.shape, 0)
        row = lax.broadcasted_iota(jnp.int32, scores.shape, 1)
        return jnp.where(key - row <= place * PR_DEV, scores, negative)
    ahead = nt(keys[:prompt_len], query)
    scores = nt(keys[prompt_len:], query)
    key = lax.broadcasted_iota(jnp.int32, scores.shape, 0)
    row = lax.broadcasted_iota(jnp.int32, scores.shape, 1)
    limit = jnp.where(key < half_len, row + place % 2 - 1, row + half_len)
    return jnp.concatenate([ahead, jnp.where(key <= limit, scores, negative)], 0)


def attend_kernel(axis_sizes, group, prompt_len, q_ref, kv_ref, out_ref, log_ref):
    place = lax.axis_index("z") * axis_sizes + lax.axis_index("x")
    tok_rows = q_ref.shape[1]
    half_len = tok_rows - PR_DEV
    kv_heads = kv_ref.shape[2] // (2 * HS)
    for kv_head in range(kv_heads):
        keys = kv_ref[0, :, kv_head * HS : (kv_head + 1) * HS]
        values = kv_ref[0, :, (kv_heads + kv_head) * HS : (kv_heads + kv_head + 1) * HS]
        values_t = values.T
        for member in range(group):
            head = kv_head * group + member
            for first, rows in ((0, PR_DEV), (PR_DEV, half_len)):
                query = q_ref[0, first : first + rows, head * HS : (head + 1) * HS]
                scores = masked_scores(place, keys, query, rows, first, prompt_len, half_len)
                row_max = jnp.max(scores, 0, keepdims=True)
                weight = jnp.exp(scores - row_max)
                total = jnp.sum(weight, 0, keepdims=True)
                mixed = nn(values_t[:, : scores.shape[0]], weight.astype(bf16)) / total
                out_ref[0, first : first + rows, head * HS : (head + 1) * HS] = mixed.T.astype(bf16)
                log_ref[0, head : head + 1, first : first + rows] = row_max + jnp.log(total)


def attend_back_kernel(
    axis_sizes, group, prompt_len, q_ref, kv_ref, grad_ref, log_ref, dq_ref, dkv_ref
):
    place = lax.axis_index("z") * axis_sizes + lax.axis_index("x")
    tok_rows = q_ref.shape[1]
    half_len = tok_rows - PR_DEV
    kv_heads = kv_ref.shape[2] // (2 * HS)
    for kv_head in range(kv_heads):
        key_cols = slice(kv_head * HS, (kv_head + 1) * HS)
        value_cols = slice((kv_heads + kv_head) * HS, (kv_heads + kv_head + 1) * HS)
        keys = kv_ref[0, :, key_cols]
        values = kv_ref[0, :, value_cols]
        keys_t = keys.T
        grad_keys = [0.0, 0.0]
        grad_values = [0.0, 0.0]
        for member in range(group):
            head = kv_head * group + member
            for part, (first, rows) in enumerate(((0, PR_DEV), (PR_DEV, half_len))):
                cols = slice(head * HS, (head + 1) * HS)
                query = q_ref[0, first : first + rows, cols]
                grad = grad_ref[0, first : first + rows, cols]
                scores = masked_scores(place, keys, query, rows, first, prompt_len, half_len)
                probs = jnp.exp(scores - log_ref[0, head : head + 1, first : first + rows])
                count = scores.shape[0]
                grad_probs = nt(values[:count], grad)
                delta = jnp.sum(probs * grad_probs, 0, keepdims=True)
                grad_scores = (probs * (grad_probs - delta)).astype(bf16)
                grad_values[part] += nn(probs.astype(bf16), grad)
                grad_keys[part] += nn(grad_scores, query)
                dq = nn(keys_t[:, :count], grad_scores) * HS ** (-0.5)
                dq_ref[0, first : first + rows, cols] = dq.T
        for cols, parts in ((key_cols, grad_keys), (value_cols, grad_values)):
            dkv_ref[0, :prompt_len, cols] = (parts[0] + parts[1][:prompt_len]).astype(bf16)
            dkv_ref[0, prompt_len:, cols] = parts[1][prompt_len:].astype(bf16)


def whole_block(shape):
    return pl.BlockSpec((1,) + shape[1:], lambda step: (step, 0, 0))


def attend(queries, all_kv, group, prompt_len):
    count, tok_rows, width = queries.shape
    keys = all_kv.shape[1]
    heads = count * width // HS
    log_shape = (count, width // HS, tok_rows)
    return pl.pallas_call(
        functools.partial(attend_kernel, lax.axis_size("x"), group, prompt_len),
        grid=(count,),
        in_specs=[whole_block(queries.shape), whole_block(all_kv.shape)],
        out_specs=[whole_block(queries.shape), whole_block(log_shape)],
        out_shape=[
            jax.ShapeDtypeStruct(queries.shape, bf16),
            jax.ShapeDtypeStruct(log_shape, f32),
        ],
        cost_estimate=pl.CostEstimate(
            flops=16 * heads * tok_rows * keys * HS,
            transcendentals=heads * tok_rows * keys,
            bytes_accessed=8 * queries.size + 2 * all_kv.size,
        ),
        compiler_params=pltpu.CompilerParams(vmem_limit_bytes=48 << 20),
        name="attend",
    )(queries, all_kv)


def attend_back(queries, all_kv, grads, logs, group, prompt_len):
    count, tok_rows, width = queries.shape
    keys = all_kv.shape[1]
    heads = count * width // HS
    return pl.pallas_call(
        functools.partial(attend_back_kernel, lax.axis_size("x"), group, prompt_len),
        grid=(count,),
        in_specs=[whole_block(value.shape) for value in (queries, all_kv, grads, logs)],
        out_specs=[whole_block(queries.shape), whole_block(all_kv.shape)],
        out_shape=[
            jax.ShapeDtypeStruct(queries.shape, f32),
            jax.ShapeDtypeStruct(all_kv.shape, bf16),
        ],
        cost_estimate=pl.CostEstimate(
            flops=40 * heads * tok_rows * keys * HS,
            transcendentals=heads * tok_rows * keys,
            bytes_accessed=12 * queries.size + 6 * all_kv.size,
        ),
        compiler_params=pltpu.CompilerParams(vmem_limit_bytes=56 << 20),
        name="attend_back",
    )(queries, all_kv, grads, logs)


def body(
    hidden_in,
    cotangent,
    routes,
    attn_gain,
    q_weight,
    k_weight,
    v_weight,
    o_weight,
    ffn_gain,
    router_weight,
    gate_weight,
    up_weight,
    down_weight,
):
    tok_rows, model_width = hidden_in.shape
    odd = lax.axis_index("x")
    shard_pos = lax.axis_index(SHARD)
    expert_pos = lax.axis_index(EXPERT)
    expert_size = lax.axis_size(EXPERT)
    shards = lax.axis_size(SHARD)
    pairs = lax.axis_size("z")
    experts_here, shard_rows, inner_width = gate_weight.shape
    experts_all = router_weight.shape[1]
    piece = inner_width // shards
    half_width = inner_width // 2
    half_len = tok_rows - PR_DEV
    prompt_len = PR_DEV * shards
    q_cols = q_weight.shape[1] // expert_size
    k_cols = k_weight.shape[1] // expert_size
    o_cols = o_weight.shape[1] // expert_size
    group = q_weight.shape[1] // k_weight.shape[1]
    qkv_cols = q_cols + 2 * k_cols

    def columns_here(weight):
        width = weight.shape[1] // expert_size
        return lax.dynamic_slice_in_dim(weight, expert_pos * width, width, 1)

    small = jnp.concatenate(
        [
            attn_gain[:, None],
            ffn_gain[:, None],
            router_weight,
            jnp.zeros((shard_rows, 126 - experts_all), bf16),
        ],
        1,
    )
    first_shard = jnp.concatenate(
        [
            columns_here(q_weight),
            columns_here(k_weight),
            columns_here(v_weight),
            columns_here(o_weight),
            small,
        ],
        1,
    )
    everyone = EXPERT + SHARD
    first_all = lax.all_gather(first_shard, everyone, axis=0, tiled=True)
    first_all = first_all.reshape(expert_size, model_width, qkv_cols + o_cols + 128)
    w_qkv = first_all[:, :, :qkv_cols]
    w_out = first_all[:, :, qkv_cols : qkv_cols + o_cols]
    small_all = first_all[0, :, qkv_cols + o_cols :]
    gain_one = small_all[:, 0].astype(f32)
    gain_two = small_all[:, 1].astype(f32)
    w_router = small_all[:, 2 : 2 + experts_all]

    def halves(weight):
        cut = weight.reshape(experts_here, shard_rows, pairs, 2, piece)
        cut = cut.transpose(3, 1, 2, 0, 4).reshape(2, shard_rows, experts_here * half_width)
        return cut

    both = jnp.concatenate([halves(gate_weight), halves(up_weight)], 2)
    kept, given = pick(odd, both[1], both[0]), pick(odd, both[0], both[1])
    received = other(given, "x")
    mine = jnp.concatenate([pick(odd, received, kept), pick(odd, kept, received)], 0)
    w_gate_up = lax.all_gather(mine, "z", axis=0, tiled=True)
    w_down = lax.all_gather(
        down_weight.reshape(experts_here * piece, model_width), "z", axis=0, tiled=True
    )
    cot_all = gather_tokens(cotangent)

    row_index = jnp.arange(tok_rows, dtype=jnp.int32)
    positions = jnp.where(
        row_index < PR_DEV,
        shard_pos * PR_DEV + row_index,
        prompt_len + 2 * (row_index - PR_DEV) + odd,
    )
    q_cos, q_sin = rope_tables(positions, q_cols)
    k_cos, k_sin = q_cos[:, :k_cols], q_sin[:, :k_cols]
    x_float = hidden_in.astype(f32)
    normed_one, inverse_one, scaled_one = norm_rows(x_float, gain_one)
    attn_input = scaled_one.astype(bf16)
    lin = jnp.einsum("td,qdc->qtc", attn_input, w_qkv, preferred_element_type=f32)
    q_lin, k_lin, v_lin = (
        lin[:, :, :q_cols],
        lin[:, :, q_cols : q_cols + k_cols],
        lin[:, :, q_cols + k_cols :],
    )
    queries = (q_lin * q_cos + rotated(q_lin) * q_sin).astype(bf16) * bf16(HS ** (-0.5))
    keys = (k_lin * k_cos + rotated(k_lin) * k_sin).astype(bf16)
    kv = jnp.concatenate([keys, v_lin.astype(bf16)], 2)
    kv_flat = kv.transpose(1, 0, 2).reshape(tok_rows, expert_size * 2 * k_cols)
    prompt_kv = lax.all_gather(kv_flat[:PR_DEV], SHARD, axis=0, tiled=True)
    partner_kv = other(kv_flat[PR_DEV:], "x")
    all_kv = jnp.concatenate([prompt_kv, partner_kv, kv_flat[PR_DEV:]], 0)
    all_kv = all_kv.reshape(-1, expert_size, 2 * k_cols).transpose(1, 0, 2)
    mix_blocks, logs = attend(queries, all_kv, group, prompt_len)
    attn_mix = mix_blocks.transpose(1, 0, 2).reshape(tok_rows, -1)
    branch = jnp.concatenate([nn(attn_mix, w_out[place]) for place in range(expert_size)], 1)
    residual = x_float + branch
    normed_two, inverse_two, scaled_two = norm_rows(residual, gain_two)
    ffn_input = scaled_two.astype(bf16)

    logits = nn(ffn_input, w_router)
    expert_ids = jnp.arange(experts_all, dtype=jnp.int32)
    taken = jnp.any(routes[:, :, None] == expert_ids[None, None, :], 1)
    masked = jnp.where(taken, logits, negative)
    raised = jnp.where(taken, jnp.exp(masked - jnp.max(masked, -1, keepdims=True)), 0.0)
    gates = raised / jnp.sum(raised, -1, keepdims=True)
    gates_high = gates.astype(bf16)
    gates_low = (gates - gates_high.astype(f32)).astype(bf16)
    lanes = jnp.arange(128, dtype=jnp.int32)[None, :]
    placed = nn(gates_high, (lanes == expert_ids[:, None]).astype(bf16)) + nn(
        gates_low, (lanes == experts_all + expert_ids[:, None]).astype(bf16)
    )
    sent = jnp.concatenate([ffn_input, placed.astype(bf16)], 1)
    token_all = gather_tokens(sent)
    rows_all = token_all[:, :model_width]

    width = experts_here * half_width
    column_expert = jnp.arange(width, dtype=jnp.int32) // piece % experts_here
    column_expert = column_expert + expert_pos * experts_here
    source = jnp.arange(128, dtype=jnp.int32)[:, None]
    to_columns = (source == column_expert[None, :]) | (
        source == experts_all + column_expert[None, :]
    )
    spread = nn(token_all[:, model_width:], to_columns.astype(bf16))
    gate_up = nn(rows_all, w_gate_up)
    gate_proj, up_proj = gate_up[:, :width], gate_up[:, width:]
    sig_gate = jax.nn.sigmoid(gate_proj)
    silu_gate = gate_proj * sig_gate
    inner_act = (silu_gate * up_proj).astype(bf16).astype(f32)
    gated = (inner_act * spread).astype(bf16)
    term_down = tn(gated, cot_all).astype(bf16)
    w_down, term_down = lax.optimization_barrier((w_down, term_down))
    grad_plain = nt(cot_all, w_down)
    extra = -(-4 * experts_all // 128) * 128
    target = jnp.arange(extra, dtype=jnp.int32)[None, :]
    from_columns = (target == odd * experts_all + column_expert[:, None]) | (
        target == (2 + odd) * experts_all + column_expert[:, None]
    )
    gates_grad = nn((inner_act * grad_plain).astype(bf16), from_columns.astype(bf16))
    grads_high = gates_grad.astype(bf16)
    grads_low = (gates_grad - grads_high.astype(f32)).astype(bf16)
    returned = jnp.where(target < 2 * experts_all, grads_high, grads_low)
    grad_inner = grad_plain * spread
    grad_gate_proj = (
        grad_inner * up_proj * sig_gate * (1.0 + gate_proj * (1.0 - sig_gate))
    ).astype(bf16)
    grad_up_proj = (grad_inner * silu_gate).astype(bf16)
    grad_both = jnp.concatenate([grad_gate_proj, grad_up_proj], 1)

    def back_rows(start, stop):
        rows = nt(grad_both[start:stop], w_gate_up).astype(bf16)
        return jnp.concatenate([rows, returned[start:stop]], 1)

    back = reduce_tokens(back_rows, rows_all.shape[0])
    back, gates_back = back[:, :model_width], back[:, model_width:]
    grad_down = lax.psum_scatter(term_down, "z", scatter_dimension=0, tiled=True)
    grad_down = grad_down.astype(f32).reshape(experts_here, piece, model_width)
    term_gate = tn(rows_all, grad_gate_proj).astype(bf16)
    term_up = tn(rows_all, grad_up_proj).astype(bf16)

    def from_both_halves(term):
        summed = lax.psum_scatter(term, "z", scatter_dimension=0, tiled=True)
        upper, lower = summed[:shard_rows], summed[shard_rows:]
        kept, given = pick(odd, lower, upper), pick(odd, upper, lower)
        received = other(given, "x")
        sides = jnp.stack([pick(odd, received, kept), pick(odd, kept, received)])
        sides = sides.astype(f32).reshape(2, shard_rows, pairs, experts_here, piece)
        return sides.transpose(3, 1, 2, 0, 4).reshape(experts_here, shard_rows, inner_width)

    grad_gate = from_both_halves(term_gate)

    grad_y = cotangent.astype(f32)
    gates_back = sum(
        gates_back[:, part * experts_all : (part + 1) * experts_all] for part in range(4)
    )
    centered = gates_back - jnp.sum(gates_back * gates, -1, keepdims=True)
    grad_logits = (gates * centered).astype(bf16)
    grad_ffn_input = back + nt(grad_logits, w_router)
    term_router = tn(ffn_input, grad_logits)
    grad_resid_norm, term_gain_two = norm_back(grad_ffn_input, normed_two, inverse_two, gain_two)
    grad_residual = grad_y + grad_resid_norm
    grad_branch = grad_residual.astype(bf16)
    branch_blocks = grad_branch.reshape(tok_rows, expert_size, o_cols).transpose(1, 0, 2)
    grad_mix = jnp.einsum("qtd,qcd->tc", branch_blocks, w_out, preferred_element_type=f32)
    grad_mix = grad_mix.astype(bf16).reshape(tok_rows, expert_size, q_cols).transpose(1, 0, 2)

    inputs_all = gather_experts(attn_input).reshape(-1, model_width)
    mixes_all = gather_experts(attn_mix).reshape(-1, model_width)
    grad_mix, term_gate_done, term_up, inputs_all, mixes_all = lax.optimization_barrier(
        (grad_mix, term_gate, term_up, inputs_all, mixes_all)
    )
    grad_queries, grad_kv = attend_back(queries, all_kv, grad_mix, logs, group, prompt_len)
    grad_kv = grad_kv.transpose(1, 0, 2).reshape(-1, expert_size * 2 * k_cols)
    prompt_grad = lax.psum_scatter(
        grad_kv[:prompt_len], SHARD, scatter_dimension=0, tiled=True
    ).astype(f32)
    gated, grad_kv = lax.optimization_barrier((gated, grad_kv))
    mixture = reduce_tokens(
        lambda start, stop: nn(gated[start:stop], w_down).astype(bf16), rows_all.shape[0]
    )
    hidden_out = (residual + mixture).astype(bf16)
    term_up, prompt_grad = lax.optimization_barrier((term_up, prompt_grad))
    grad_up = from_both_halves(term_up)
    partner_grad = other(grad_kv[prompt_len : prompt_len + half_len], "x").astype(f32)
    own_grad = grad_kv[prompt_len + half_len :].astype(f32) + partner_grad
    own_grad = jnp.concatenate([prompt_grad, own_grad], 0)
    own_grad = own_grad.reshape(tok_rows, expert_size, 2 * k_cols).transpose(1, 0, 2)
    grad_keys, grad_values = own_grad[:, :, :k_cols], own_grad[:, :, k_cols:]
    grad_lin = jnp.concatenate(
        [
            grad_queries * q_cos - rotated(grad_queries * q_sin),
            grad_keys * k_cos - rotated(grad_keys * k_sin),
            grad_values,
        ],
        2,
    ).astype(bf16)
    grad_attn_input = jnp.einsum("qtc,qdc->td", grad_lin, w_qkv, preferred_element_type=f32)
    grad_x_norm, term_gain_one = norm_back(grad_attn_input, normed_one, inverse_one, gain_one)
    grad_hidden = (grad_residual + grad_x_norm).astype(bf16)

    lin_all = spread_experts(grad_lin).reshape(-1, qkv_cols)
    branch_all = spread_experts(branch_blocks).reshape(-1, o_cols)
    term_qkv = tn(inputs_all, lin_all)
    term_out = tn(mixes_all, branch_all)
    gains = jnp.concatenate(
        [term_gain_one[None], term_gain_two[None], jnp.zeros((126, model_width), f32)], 0
    )
    shift = (lanes == 2 + expert_ids[:, None]).astype(bf16)
    small_terms = gains.T.astype(bf16) + nn(term_router.astype(bf16), shift).astype(bf16)
    terms = jnp.concatenate([term_qkv.astype(bf16), term_out.astype(bf16), small_terms], 1)
    terms = lax.psum_scatter(terms, SHARD, scatter_dimension=0, tiled=True)
    stacked = gather_experts(terms)
    blocks = [block.astype(f32) for block in absolute_order(stacked)]

    def columns(start, width):
        return jnp.concatenate([block[:, start : start + width] for block in blocks], 1)

    tail = sum(block[:, qkv_cols + o_cols :] for block in blocks)
    return (
        hidden_out,
        grad_hidden,
        tail[:, 0],
        columns(0, q_cols),
        columns(q_cols, k_cols),
        columns(q_cols + k_cols, k_cols),
        columns(qkv_cols, o_cols),
        tail[:, 1],
        tail[:, 2 : 2 + experts_all],
        grad_gate,
        grad_up,
        grad_down,
    )


def solution(mesh):
    devices = mesh.devices
    expert_size, shards = devices.shape
    fine = Mesh(
        devices.reshape(expert_size // 2, 2, shards // 2, 2), EXPERT + SHARD
    )
    rows = P(EXPERT + SHARD, None)
    vector, matrix = P(SHARD), P(SHARD, None)
    experts = P(EXPERT, SHARD, None)
    return jax.shard_map(
        body,
        mesh=fine,
        in_specs=(
            rows,
            rows,
            rows,
            vector,
            matrix,
            matrix,
            matrix,
            matrix,
            vector,
            matrix,
            experts,
            experts,
            experts,
        ),
        out_specs=(
            rows,
            rows,
            vector,
            matrix,
            matrix,
            matrix,
            matrix,
            vector,
            matrix,
            experts,
            experts,
            experts,
        ),
        check_vma=False,
    )
```
